32 devices in a mesh: groups: 2 (over x), mesh: 16 (over z, y, core).
Axes of the slice: x: 2, y: 2, z: 4, core: 2. Of those that a mesh axis runs over, the one named last changes fastest.
Arguments:
- state: float32 [3, 64, 32768], P(None, None, ('groups', 'mesh')), parts along dimension 2, may hold values from -6 to 6
- depth: float32 [32768], P(('groups', 'mesh')), parts along dimension 0, may hold values from 0.5 to 4
- coef: float32 [2, 6, 32768], P(None, None, ('groups', 'mesh')), parts along dimension 2, may hold values from -2 to 2
- wet_faces: int32 [6, 32768], P(None, ('groups', 'mesh')), parts along dimension 1, may hold values 0 or 1
- conn: int32 [6, 32768], P(None, ('groups', 'mesh')), parts along dimension 1, may hold values from 0 to 1535, as said below
- send_list: int32 [2, 8192], P(None, ('groups', 'mesh')), parts along dimension 1, may hold values from 0 to 1023, as said below
- obs_nodes: int32 [3, 32768], P(None, ('groups', 'mesh')), parts along dimension 1, may hold values from 0 to 1023
- obs_weight: float32 [3, 32768], P(None, ('groups', 'mesh')), parts along dimension 1, may hold values from 0 to 1, as said below
- obs_value: float32 [32768], P(('groups', 'mesh')), parts along dimension 0, may hold values from -9 to 9
- obs_error: float32 [32768], P(('groups', 'mesh')), parts along dimension 0, may hold values from 0.5 to 2
- loc_ids: int32 [32, 512], P(('groups', 'mesh')), parts along dimension 0, may hold values from 0 to 16383, as said below
- loc_len: int32 [32], P(('groups', 'mesh')), parts along dimension 0, may hold values from 64 to 512, as said below
- loc_weight: float32 [32, 512], P(('groups', 'mesh')), parts along dimension 0, may hold values from 0.05 to 1
Outputs:
- analysis: float32 [3, 64, 32768], P(None, None, ('groups', 'mesh')), parts along dimension 2
The draws below stay inside these ranges and needn't reach their ends.
There are 2 independent parts, one for each index of `groups`. The reference program is written for one: setup_inputs(seed, part) draws one part's arguments, and reference() takes and returns one part's arrays. A program takes and returns all parts, laid end to end along the dimension named above; each array names one. Nothing has to cross between parts.
Inputs may be any that keep to these rules, and one draw needn't show every extreme that they name: `conn`: for each partition: below 1024 a local node; 1024 + p is slot p of the lower partition's list toward it, 1280 + p slot p of the higher partition's list toward it; the first partition names no lower slot and the last no higher one. `send_list`: each partition's two lists hold 256 distinct local node numbers each. `obs_weight`: the three weights of an observation are positive and sum to one. `loc_ids`: the entries of a patch's list are distinct and name observations held by the patch's partition or the two beside it. `loc_len`: patch 0 has a list of length 512.
All inputs are finite; a program needn't handle non-finite values. No bound on the sum of `wet_faces` on one device may be relied on, other than what follows from the above.
Results may differ from the reference program's by a relative error of at most 0.0003.
Values sent between devices are 32-bit elements; how exact they have to be, the bound alone decides.
A program may use at most 64 MiB of HBM per device.

```python
import math
import jax
import jax.numpy as jnp
from jax import lax

MEM = 64
NB = 6
VERTICES_PER_AREA = 1024
PATCH_DEV = 1
HALO = 256
OBS_DEV = 1024
LOC = 512
STEPS = 2
NODE_DEV = 1024
NODES = 16384
ASSIMILATE_AREAS = 16
OBS = 16384
N_MESH = 16


def draw_conn(key, part):
    column = jnp.arange(NODES, dtype=jnp.int32)
    device = column // NODE_DEV
    local = column % NODE_DEV
    keys = jax.random.split(jax.random.fold_in(key, 11), 3)
    kind = jax.random.randint(keys[0], (NB, NODES), 0, 8)
    offset = jax.random.randint(keys[1], (NB, NODES), -16, 17)
    place = jax.random.randint(keys[2], (NB, NODES), 0, HALO)
    nearby = jnp.clip(local[None, :] + offset, 0, NODE_DEV - 1)
    lower_ok = (kind == 0) & (device[None, :] > 0)
    upper_ok = (kind == 1) & (device[None, :] < N_MESH - 1)
    assimilated_output = jnp.where(lower_ok, NODE_DEV + place, jnp.where(upper_ok, NODE_DEV + HALO + place, nearby))
    return assimilated_output.astype(jnp.int32)


def draw_send_list(key, part):
    keys = jax.random.split(jax.random.fold_in(key, 23), 2 * N_MESH)
    lists = jax.vmap(lambda single: jax.random.permutation(single, NODE_DEV)[:HALO])(keys)
    return lists.reshape(2, N_MESH * HALO).astype(jnp.int32)


def draw_obs_weight(key, part):
    inner = jax.random.fold_in(key, 53)
    raw = jax.random.uniform(inner, (3, OBS), jnp.float32, 0.2, 1.0)
    return raw / jnp.sum(raw, axis=0, keepdims=True)


def draw_loc_ids(key, part):
    width = 3 * OBS_DEV
    keys = jax.random.split(jax.random.fold_in(key, 37), ASSIMILATE_AREAS)
    device = jnp.arange(ASSIMILATE_AREAS, dtype=jnp.int32) // PATCH_DEV

    def single(subkey, owner):
        ranks = jax.random.permutation(subkey, width).astype(jnp.int32)
        candidate = jnp.arange(width, dtype=jnp.int32)
        target = owner + candidate // OBS_DEV - 1
        outside = ((target < 0) | (target >= N_MESH)).astype(jnp.int32)
        order = jnp.argsort(ranks + outside * width).astype(jnp.int32)
        return (owner - 1) * OBS_DEV + order[:LOC]
    return jax.vmap(single)(keys, device).astype(jnp.int32)


def draw_loc_len(key, part):
    lengths = jax.random.randint(jax.random.fold_in(key, 41), (ASSIMILATE_AREAS,), LOC // 8, LOC + 1)
    first = jnp.arange(ASSIMILATE_AREAS, dtype=jnp.int32) == 0
    return jnp.where(first, LOC, lengths).astype(jnp.int32)


def place_ends(drawn, key, least, largest):
    shape = drawn.shape
    spot = [jax.random.randint(jax.random.fold_in(key, axis), (), 0, shape[axis]) for axis in range(len(shape))]
    drawn = drawn.at[tuple(spot)].set(least)
    longest = shape.index(max(shape))
    spot[longest] = (spot[longest] + 1) % shape[longest]
    return drawn.at[tuple(spot)].set(largest)


def block_levels(own_key, extent, cuts, least, top_value):
    def one(position, blocks):
        steps = jax.random.uniform(jax.random.fold_in(jax.random.fold_in(own_key, 6), position), (blocks,), jnp.float32, least / len(cuts), top_value / len(cuts))
        return jnp.repeat(jnp.exp(steps), extent[position] // blocks).reshape((-1,) + (1,) * (len(extent) - position - 1))

    factor_of = one(*cuts[0])
    for cut in cuts[1:]:
        factor_of = factor_of * one(*cut)
    return factor_of


def scatter_about(own_key, extent, scale, reach, cuts=(), held_as=jnp.bfloat16):
    values = jax.random.normal(own_key, extent, jnp.float32) * scale
    if len(cuts) > 0:
        values = block_levels(own_key, extent, cuts, -0.22, 0.18) * values
    return jnp.clip(values, min=-reach, max=reach).astype(held_as)


def setup_inputs(seed: int = 0, part: int = 0) -> dict:
    seeds = jax.random.split(jax.random.key(seed), 14)
    own_keys = jax.random.split(jax.random.fold_in(seeds[13], part), 14)
    return {
        "state": scatter_about(own_keys[0], (3, MEM, NODES), 1.0, 6.0, ((2, 16),), jnp.float32),
        "depth": jnp.clip(jnp.exp(math.log(4.0) - 2.0794415 * jax.random.uniform(own_keys[1], (NODES,), jnp.float32) ** block_levels(own_keys[1], (NODES,), ((0, 16),), -0.2, 0.2)), 0.5, 4.0),
        "coef": scatter_about(own_keys[2], (2, NB, NODES), 0.4, 2.0, ((2, 16),), jnp.float32),
        "wet_faces": place_ends((jax.random.randint(own_keys[3], (NB, NODES), 0, 8) < 7).astype(jnp.int32), jax.random.fold_in(own_keys[3], 1), 0, 1),
        "conn": draw_conn(jax.random.fold_in(jax.random.fold_in(seeds[13], part), 71), part),
        "send_list": draw_send_list(jax.random.fold_in(jax.random.fold_in(seeds[13], part), 71), part),
        "obs_nodes": place_ends(jax.random.randint(own_keys[6], (3, OBS), 0, NODE_DEV), jax.random.fold_in(own_keys[6], 1), 0, NODE_DEV - 1).astype(jnp.int32),
        "obs_weight": draw_obs_weight(jax.random.fold_in(jax.random.fold_in(seeds[13], part), 71), part),
        "obs_value": scatter_about(own_keys[8], (OBS,), 1.5, 9.0, ((0, 16),), jnp.float32),
        "obs_error": jnp.clip(jnp.exp(math.log(2.0) - 1.3862944 * jax.random.uniform(own_keys[9], (OBS,), jnp.float32) ** block_levels(own_keys[9], (OBS,), ((0, 16),), -0.2, 0.2)), 0.5, 2.0),
        "loc_ids": draw_loc_ids(jax.random.fold_in(jax.random.fold_in(seeds[13], part), 71), part),
        "loc_len": draw_loc_len(jax.random.fold_in(jax.random.fold_in(seeds[13], part), 71), part),
        "loc_weight": jnp.clip(0.05 + 0.95 * jax.random.uniform(own_keys[12], (ASSIMILATE_AREAS, LOC), jnp.float32) ** block_levels(own_keys[12], (ASSIMILATE_AREAS, LOC), ((0, 16),), -0.2, 0.2), 0.05, 1.0),
    }


DT = 0.1
TOPMOST = lax.Precision.HIGHEST

def spread(field, lists):
    lead = field.shape[:-2]

    def pick(chosen):
        return jnp.take_along_axis(field, jnp.broadcast_to(chosen, lead + chosen.shape), axis=-1)
    to_lower = pick(lists[0])
    to_upper = pick(lists[1])
    blank = jnp.zeros_like(to_lower[..., :1, :])
    from_lower = jnp.concatenate([blank, to_upper[..., :-1, :]], axis=-2)
    from_upper = jnp.concatenate([to_lower[..., 1:, :], blank], axis=-2)
    return jnp.concatenate([field, from_lower, from_upper], axis=-1)

def fetch(extended, chosen):
    lead = extended.shape[:-2]
    return jnp.take_along_axis(extended, jnp.broadcast_to(chosen, lead + chosen.shape), axis=-1)

def mapping_operator(advance_prior_model, collected_lines, departure_lines, coefficient_lines):
    ensemble_fields = collected_lines.shape[0]
    prior_average = lax.optimization_barrier(jnp.mean(advance_prior_model, axis=1, keepdims=True))
    dispersion_piece = advance_prior_model - prior_average
    weighted = collected_lines * coefficient_lines[None]
    inner_product_table = jnp.einsum('mpl,npl->pmn', weighted, collected_lines, precision=TOPMOST)
    unit = jnp.eye(ensemble_fields, dtype=jnp.float32)
    inner_product_table = inner_product_table + (ensemble_fields - 1.0) * unit
    linear_system_source = jnp.einsum('mpl,pl->pm', collected_lines, coefficient_lines * departure_lines, precision=TOPMOST)
    lower = jnp.linalg.cholesky(inner_product_table)
    inv_lower = lax.linalg.triangular_solve(lower, jnp.broadcast_to(unit, inner_product_table.shape), left_side=True, lower=True)
    halfway = lax.linalg.triangular_solve(lower, linear_system_source[..., None], left_side=True, lower=True)
    mean_w = lax.linalg.triangular_solve(lower, halfway, left_side=True, lower=True, transpose_a=True)[..., 0]
    blending_coefficients = mean_w[:, :, None] + math.sqrt(ensemble_fields - 1.0) * jnp.swapaxes(inv_lower, 1, 2)
    return prior_average + jnp.einsum('hwz,vwhx->vzhx', blending_coefficients, dispersion_piece, precision=TOPMOST)

def reference(state, depth, coef, wet_faces, conn, send_list, obs_nodes, obs_weight, obs_value, obs_error, loc_ids, loc_len, loc_weight):
    ensemble_fields = state.shape[1]
    parts = N_MESH
    shaped = state.reshape(3, ensemble_fields, parts, NODE_DEV)
    free_elevation = shaped[0]
    discharge_rate = shaped[1:]
    lists = send_list.reshape(2, parts, HALO)
    links = conn.reshape(NB, parts, NODE_DEV)
    faces = wet_faces.astype(jnp.float32).reshape(NB, parts, NODE_DEV)
    slopes = coef.reshape(2, NB, parts, NODE_DEV)
    height = depth.reshape(parts, NODE_DEV)
    for section in range(STEPS):
        extended = spread(discharge_rate, lists)
        divergence = jnp.zeros_like(free_elevation)
        for slot in range(NB):
            nearby = fetch(extended, links[slot])
            divergence = divergence + faces[slot] * (slopes[0, slot] * (nearby[0] - discharge_rate[0]) + slopes[1, slot] * (nearby[1] - discharge_rate[1]))
        free_elevation = free_elevation - DT * height * divergence
        ext_level = spread(free_elevation, lists)
        slope_east = jnp.zeros_like(free_elevation)
        slope_north = jnp.zeros_like(free_elevation)
        for slot in range(NB):
            change = fetch(ext_level, links[slot]) - free_elevation
            slope_east = slope_east + faces[slot] * slopes[0, slot] * change
            slope_north = slope_north + faces[slot] * slopes[1, slot] * change
        discharge_rate = jnp.stack([discharge_rate[0] - DT * slope_east, discharge_rate[1] - DT * slope_north])
    flat_level = free_elevation.reshape(ensemble_fields, NODES)
    owners = jnp.arange(OBS, dtype=jnp.int32) // OBS_DEV * NODE_DEV
    observed = jnp.zeros((ensemble_fields, OBS), jnp.float32)
    for corner in range(3):
        observed = observed + obs_weight[corner] * jnp.take(flat_level, obs_nodes[corner] + owners, axis=1)
    obs_mean = lax.optimization_barrier(jnp.mean(observed, axis=0))
    anomalies = observed - obs_mean
    innovation = obs_value - obs_mean
    numeric_accuracy = 1.0 / (obs_error * obs_error)
    collected_lines = jnp.take(anomalies, loc_ids, axis=1)
    departure_lines = jnp.take(innovation, loc_ids, axis=0)
    prec_list = jnp.take(numeric_accuracy, loc_ids, axis=0)
    live = (jnp.arange(LOC, dtype=jnp.int32)[None, :] < loc_len[:, None]).astype(jnp.float32)
    coefficient_lines = prec_list * loc_weight * live
    advance_prior_model = jnp.stack([free_elevation, discharge_rate[0], discharge_rate[1]]).reshape(3, ensemble_fields, ASSIMILATE_AREAS, VERTICES_PER_AREA)
    assimilated_output = mapping_operator(advance_prior_model, collected_lines, departure_lines, coefficient_lines)
    return assimilated_output.reshape(3, ensemble_fields, NODES)
```

```python
import functools
import math

import jax
import jax.numpy as jnp
from jax import lax
from jax.experimental import pallas as pl
from jax.experimental.pallas import tpu as pltpu
from jax.sharding import PartitionSpec as P

STEPS = 2
DT = 0.1
TOPMOST = lax.Precision.HIGHEST
LANES = 128
CHUNK = 256
F32, BF16 = jnp.float32, jnp.bfloat16


def halves(x):
    high = x.astype(BF16)
    return high, (x - high.astype(F32)).astype(BF16)


def dot(a, b):
    return jnp.dot(a, b, preferred_element_type=F32)


def merge_slots(ids, weights):
    ids, weights = list(ids), [list(w) for w in weights]
    for s in range(1, len(ids)):
        for t in range(s):
            same = ids[s] == ids[t]
            for w in weights:
                w[t] = w[t] + jnp.where(same, w[s], 0.0)
            ids[s] = jnp.where(same, -1, ids[s])
    return ids, weights


def build(out_ref, places, extent, ids_ref, parts_ref, slots, kinds):
    columns = ids_ref.shape[1]
    rows = 16

    def column(c, _):
        cols = pl.ds(pl.multiple_of(c * LANES, LANES), LANES)
        ids = [jnp.broadcast_to(ids_ref[s : s + 1, cols], (rows, LANES)).astype(jnp.int16) for s in range(slots)]
        parts = [
            [jnp.broadcast_to(parts_ref[q * slots + s : q * slots + s + 1, cols], (rows, LANES)).astype(BF16) for s in range(slots)]
            for q in range(kinds)
        ]
        blank = jnp.zeros((rows, LANES), BF16)

        unroll = 4

        def block(r, _):
            for u in range(unroll):
                start = pl.multiple_of((r * unroll + u) * rows, rows)
                here = places + jnp.full((rows, LANES), start, jnp.int32).astype(jnp.int16)
                total = [blank] * kinds
                for s in range(slots):
                    hit = here == ids[s]
                    total = [jnp.where(hit, parts[q][s], total[q]) for q in range(kinds)]
                for q in range(kinds):
                    out_ref[q, pl.ds(start, rows), cols] = total[q]
            return 0

        lax.fori_loop(0, extent // (rows * unroll), block, 0)
        return 0

    lax.fori_loop(0, columns // LANES, column, 0)


def linv_of(table, unit, members):
    width = 8
    work = jnp.concatenate([table, unit], axis=1)
    count = members // width
    blocks = [work[b * width : (b + 1) * width] for b in range(count)]
    done = []
    for b in range(count):
        first = b * width
        panel = blocks[b]
        rows = [panel[j : j + 1] for j in range(width)]
        below = blocks[b + 1 :]
        cols = [[blk[:, first + j : first + j + 1] for blk in below] for j in range(width)]
        corner = [[panel[j : j + 1, first + i : first + i + 1] for i in range(width)] for j in range(width)]
        scaled = []
        for j in range(width):
            inverse = 1.0 / corner[j][j]
            unit_row = rows[j] * inverse
            scaled.append(unit_row)
            for i in range(j + 1, width):
                factor = corner[j][i]
                rows[i] = rows[i] - factor * unit_row
                scale = factor * inverse
                cols[i] = [ci - cj * scale for ci, cj in zip(cols[i], cols[j])]
                for k in range(i, width):
                    value = corner[i][k] - scale * corner[j][k]
                    corner[i][k] = value
                    corner[k][i] = value
        for j in range(width):
            done.append(rows[j] * lax.rsqrt(corner[j][j]))
        for n in range(len(below)):
            total = below[n]
            for j in range(width):
                total = total - cols[j][n] * scaled[j]
            blocks[b + 1 + n] = total
    return jnp.concatenate(done, axis=0)[:, members:]


def kernel(
    n, state, depth, coef, wet, conn, lists, obs_nodes, obs_weight, obs_value, obs_error, loc_ids, loc_len, loc_weight,
    out, field, operator, picker, sampler, slot_ids, slot_parts, obs_ids, obs_parts, totals, mixed, gather_mixed,
    sums, send_flow, got_flow, send_level, got_level, shares, got_shares, grams, got_grams, anomalies, send_sem, recv_sem,
):
    me = lax.axis_index("mesh")
    lower, upper = lax.rem(me + n - 1, n), lax.rem(me + 1, n)
    has_lower, has_upper = me > 0, me < n - 1
    members, nodes = state.shape[1], state.shape[2]
    slots, corners = conn.shape[0], obs_nodes.shape[0]
    width = lists.shape[1]
    extent = nodes + 2 * width
    obs_count = obs_value.shape[1]

    barrier = pltpu.get_barrier_semaphore()

    @pl.when(has_lower)
    def _():
        pl.semaphore_signal(barrier, inc=1, device_id={"mesh": lower}, device_id_type=pl.DeviceIdType.MESH)

    @pl.when(has_upper)
    def _():
        pl.semaphore_signal(barrier, inc=1, device_id={"mesh": upper}, device_id_type=pl.DeviceIdType.MESH)

    def pair(k, source, target):
        down = pltpu.make_async_remote_copy(
            src_ref=source.at[0], dst_ref=target.at[1], send_sem=send_sem.at[k, 0], recv_sem=recv_sem.at[k, 0],
            device_id={"mesh": lower}, device_id_type=pl.DeviceIdType.MESH,
        )
        up = pltpu.make_async_remote_copy(
            src_ref=source.at[1], dst_ref=target.at[0], send_sem=send_sem.at[k, 1], recv_sem=recv_sem.at[k, 1],
            device_id={"mesh": upper}, device_id_type=pl.DeviceIdType.MESH,
        )
        return down, up

    def start(copies):
        pl.when(has_lower)(copies[0].start)
        pl.when(has_upper)(copies[1].start)

    def arrive(copies):
        pl.when(has_upper)(copies[0].wait_recv)
        pl.when(has_lower)(copies[1].wait_recv)

    def sent(copies):
        pl.when(has_lower)(copies[0].wait_send)
        pl.when(has_upper)(copies[1].wait_send)

    flow_copies = [pair(i, send_flow.at[i], got_flow.at[i]) for i in range(STEPS)]
    level_copies = [pair(STEPS + i, send_level.at[i], got_level.at[i]) for i in range(STEPS)]
    share_copies = pair(2 * STEPS, shares, got_shares)
    gram_copies = pair(2 * STEPS + 1, grams, got_grams)

    def blank_side(side):
        for i in range(STEPS):
            got_flow[i, side] = jnp.zeros_like(got_flow[i, side])
            got_level[i, side] = jnp.zeros_like(got_level[i, side])
        got_shares[side] = jnp.zeros_like(got_shares[side])
        got_grams[side] = jnp.zeros_like(got_grams[side])

    pl.when(me == 0)(lambda: blank_side(0))
    pl.when(me == n - 1)(lambda: blank_side(1))

    places = lax.broadcasted_iota(jnp.int32, (16, LANES), 0).astype(jnp.int16)

    def pick_column(c, _):
        cols = pl.ds(pl.multiple_of(c * LANES, LANES), LANES)
        for h in range(2):
            ids = jnp.broadcast_to(lists[h : h + 1, cols], (16, LANES)).astype(jnp.int16)

            def block(r, _):
                begin = pl.multiple_of(r * 16, 16)
                here = places + jnp.full((16, LANES), begin, jnp.int32).astype(jnp.int16)
                picker[h, pl.ds(begin, 16), cols] = jnp.where(here == ids, jnp.ones((16, LANES), BF16), jnp.zeros((16, LANES), BF16))
                return 0

            lax.fori_loop(0, nodes // 16, block, 0, unroll=4)
        return 0

    lax.fori_loop(0, width // LANES, pick_column, 0)

    def split_field(f, values, cols):
        high, low = halves(values)
        mixed[2 * f * members : (2 * f + 1) * members, cols] = high
        mixed[(2 * f + 1) * members : (2 * f + 2) * members, cols] = low

    def send_fields(first, number, target):
        for h in range(2):
            picked = dot(mixed[2 * first * members : 2 * (first + number) * members, :], picker[h])
            for f in range(number):
                base = 2 * f * members
                target[h, f * members : (f + 1) * members, :] = (
                    picked[base : base + members] + picked[base + members : base + 2 * members]
                )

    def over_chunks(body):
        def step(c, _):
            body(pl.ds(pl.multiple_of(c * CHUNK, CHUNK), CHUNK))
            return 0

        lax.fori_loop(0, nodes // CHUNK, step, 0)

    def product(pairs_ref, base, op, rows, cols):
        both = dot(pairs_ref[base : base + 2 * members, :], operator[2 * op, rows, cols])
        cross = dot(pairs_ref[base : base + members, :], operator[2 * op + 1, rows, cols])
        return both[:members] + both[members:] + cross

    local_rows, ghost_rows = slice(0, nodes), slice(nodes, extent)

    def first_split(cols):
        for f in (1, 2):
            split_field(f, state[f, :, cols], cols)

    over_chunks(first_split)
    send_fields(1, 2, send_flow.at[0])

    pl.semaphore_wait(barrier, jnp.minimum(me, 1) + jnp.minimum(n - 1 - me, 1))
    start(flow_copies[0])

    list_size = loc_ids.shape[1]
    groups = 3 * obs_count // LANES
    live = lax.broadcasted_iota(jnp.int32, (1, list_size), 1) < loc_len[0]
    entry = jnp.where(live, loc_weight[...], 0.0)
    position = loc_ids[...] - (me - 1) * obs_count
    major, minor = position // LANES, lax.rem(position, LANES)
    coarse = jnp.where(lax.broadcasted_iota(jnp.int32, (groups, list_size), 0) == major, entry, 0.0)
    fine = jnp.where(lax.broadcasted_iota(jnp.int32, (LANES, list_size), 0) == minor, 1.0, 0.0)
    dense = lax.dot_general(coarse, fine, (((1,), (1,)), ((), ())), precision=TOPMOST, preferred_element_type=F32)
    third = groups // 3
    shares[0] = dense[:third]
    shares[1] = dense[2 * third :]
    own_share = dense[third : 2 * third]
    start(share_copies)

    faces = wet[...].astype(F32)
    east, north = faces * coef[0], faces * coef[1]
    totals[0:1] = jnp.sum(east, axis=0, keepdims=True)
    totals[1:2] = jnp.sum(north, axis=0, keepdims=True)
    ids, (east_slots, north_slots) = merge_slots(
        [conn[s : s + 1] for s in range(slots)],
        [[east[s : s + 1] for s in range(slots)], [north[s : s + 1] for s in range(slots)]],
    )
    for s in range(slots):
        slot_ids[s : s + 1] = ids[s]
        for q, w in enumerate((east_slots[s], north_slots[s])):
            high, low = halves(w)
            slot_parts[2 * q * slots + s : 2 * q * slots + s + 1] = high.astype(F32)
            slot_parts[(2 * q + 1) * slots + s : (2 * q + 1) * slots + s + 1] = low.astype(F32)
    build(operator, places, extent, slot_ids, slot_parts, slots, 4)

    ids, (weight_slots,) = merge_slots(
        [obs_nodes[s : s + 1] for s in range(corners)], [[obs_weight[s : s + 1] for s in range(corners)]]
    )
    for s in range(corners):
        obs_ids[s : s + 1] = ids[s]
        high, low = halves(weight_slots[s])
        obs_parts[s : s + 1] = high.astype(F32)
        obs_parts[corners + s : corners + s + 1] = low.astype(F32)

    for i in range(STEPS):
        old = state if i == 0 else field
        last = i == STEPS - 1

        def flow_local(cols, old=old):
            sums[0, :, cols] = (
                product(mixed, 2 * members, 0, local_rows, cols)
                + product(mixed, 4 * members, 1, local_rows, cols)
                - old[1, :, cols] * totals[0:1, cols]
                - old[2, :, cols] * totals[1:2, cols]
            )

        over_chunks(flow_local)
        if i == 0:
            build(sampler, places, nodes, obs_ids, obs_parts, corners, 2)
        arrive(flow_copies[i])
        for side in range(2):
            for f in range(2):
                high, low = halves(got_flow[i, side, f * members : (f + 1) * members, :])
                gather_mixed[2 * f * members : (2 * f + 1) * members, side * width : (side + 1) * width] = high
                gather_mixed[(2 * f + 1) * members : (2 * f + 2) * members, side * width : (side + 1) * width] = low

        def flow_ghost(cols, old=old):
            divergence = (
                sums[0, :, cols]
                + product(gather_mixed, 0, 0, ghost_rows, cols)
                + product(gather_mixed, 2 * members, 1, ghost_rows, cols)
            )
            level = old[0, :, cols] - DT * depth[0:1, cols] * divergence
            field[0, :, cols] = level
            split_field(0, level, cols)

        over_chunks(flow_ghost)
        send_fields(0, 1, send_level.at[i])
        start(level_copies[i])

        if last:
            arrive(share_copies)

            def observe(cols):
                both = dot(mixed[: 2 * members, :], sampler[0, :, cols])
                observed = both[:members] + both[members:] + dot(mixed[:members, :], sampler[1, :, cols])
                mean = jnp.mean(observed, axis=0, keepdims=True)
                anomalies[:members, cols] = observed - mean
                anomalies[members : members + 8, cols] = jnp.broadcast_to(obs_value[0:1, cols] - mean, (8, CHUNK))

            over_chunks(observe)
            precision = 1.0 / (obs_error[...] * obs_error[...])
            scaled = []
            for share in (got_shares[0], own_share, got_shares[1]):
                line = jnp.concatenate([share[a : a + 1] for a in range(third)], axis=1)
                scaled.append(anomalies[...] * (line * precision))
            table = lax.dot_general(
                jnp.concatenate(scaled, axis=0), anomalies[:members], (((1,), (1,)), ((), ())),
                precision=TOPMOST, preferred_element_type=F32,
            )
            tall = members + 8
            pad = jnp.zeros((tall, grams.shape[2] - members), F32)
            grams[0] = jnp.concatenate([table[:tall], pad], axis=1)
            grams[1] = jnp.concatenate([table[2 * tall :], pad], axis=1)
            own_table = table[tall : 2 * tall]
            start(gram_copies)

        def level_local(cols):
            level = field[0, :, cols]
            for d in range(2):
                sums[d, :, cols] = product(mixed, 0, d, local_rows, cols) - level * totals[d : d + 1, cols]

        over_chunks(level_local)
        arrive(level_copies[i])
        for side in range(2):
            high, low = halves(got_level[i, side])
            gather_mixed[:members, side * width : (side + 1) * width] = high
            gather_mixed[members : 2 * members, side * width : (side + 1) * width] = low

        def level_ghost(cols, old=old, last=last):
            for d in range(2):
                slope = sums[d, :, cols] + product(gather_mixed, 0, d, ghost_rows, cols)
                value = old[1 + d, :, cols] - DT * slope
                field[1 + d, :, cols] = value
                if not last:
                    split_field(1 + d, value, cols)

        over_chunks(level_ghost)
        if not last:
            send_fields(1, 2, send_flow.at[i + 1])
            start(flow_copies[i + 1])

    arrive(gram_copies)
    combined = own_table + got_grams[0, :, :members] + got_grams[1, :, :members]
    unit = jnp.where(
        lax.broadcasted_iota(jnp.int32, (members, members), 0) == lax.broadcasted_iota(jnp.int32, (members, members), 1), 1.0, 0.0
    )
    linv = linv_of(combined[:members] + (members - 1.0) * unit, unit, members)
    rhs = combined[members : members + 1]
    halfway = jnp.sum(linv * rhs, axis=1, keepdims=True)
    mean_w = jnp.sum(linv * halfway, axis=0, keepdims=True)
    blend = mean_w + math.sqrt(members - 1.0) * linv

    def analyse(cols):
        for c in range(3):
            forecast = field[c, :, cols]
            average = jnp.mean(forecast, axis=0, keepdims=True)
            out[c, :, cols] = average + jnp.dot(blend, forecast - average, precision=TOPMOST, preferred_element_type=F32)

    over_chunks(analyse)
    for copies in flow_copies + level_copies + [share_copies, gram_copies]:
        sent(copies)


def local(
    n, state, depth, coef, wet_faces, conn, send_list, obs_nodes, obs_weight, obs_value, obs_error, loc_ids, loc_len, loc_weight
):
    members, nodes = state.shape[1], state.shape[2]
    slots, corners, width = conn.shape[0], obs_nodes.shape[0], send_list.shape[1]
    obs_count = obs_value.shape[0]
    extent = nodes + 2 * width
    assert loc_ids.shape[0] == 1
    vmem = pl.BlockSpec(memory_space=pltpu.VMEM)
    smem = pl.BlockSpec(memory_space=pltpu.SMEM)
    number = 2 * STEPS + 2
    return pl.pallas_call(
        functools.partial(kernel, n),
        out_shape=jax.ShapeDtypeStruct(state.shape, F32),
        in_specs=[vmem] * 11 + [smem, vmem],
        out_specs=vmem,
        scratch_shapes=[
            pltpu.VMEM((3, members, nodes), F32),
            pltpu.VMEM((4, extent, nodes), BF16),
            pltpu.VMEM((2, nodes, width), BF16),
            pltpu.VMEM((2, nodes, obs_count), BF16),
            pltpu.VMEM((8, nodes), jnp.int32),
            pltpu.VMEM((4 * slots, nodes), F32),
            pltpu.VMEM((8, obs_count), jnp.int32),
            pltpu.VMEM((8, obs_count), F32),
            pltpu.VMEM((8, nodes), F32),
            pltpu.VMEM((6 * members, nodes), BF16),
            pltpu.VMEM((4 * members, 2 * width), BF16),
            pltpu.VMEM((2, members, nodes), F32),
            pltpu.VMEM((STEPS, 2, 2 * members, width), F32),
            pltpu.VMEM((STEPS, 2, 2 * members, width), F32),
            pltpu.VMEM((STEPS, 2, members, width), F32),
            pltpu.VMEM((STEPS, 2, members, width), F32),
            pltpu.VMEM((2, obs_count // LANES, LANES), F32),
            pltpu.VMEM((2, obs_count // LANES, LANES), F32),
            pltpu.VMEM((2, members + 8, LANES), F32),
            pltpu.VMEM((2, members + 8, LANES), F32),
            pltpu.VMEM((members + 8, obs_count), F32),
            pltpu.SemaphoreType.DMA((number, 2)),
            pltpu.SemaphoreType.DMA((number, 2)),
        ],
        compiler_params=pltpu.CompilerParams(collective_id=0, has_side_effects=True, vmem_limit_bytes=56 * 1024 * 1024),
    )(
        state, depth[None], coef, wet_faces, conn, send_list, obs_nodes, obs_weight, obs_value[None], obs_error[None],
        loc_ids, loc_len, loc_weight,
    )


def solution(mesh):
    split = ("groups", "mesh")
    in_specs = (
        P(None, None, split), P(split), P(None, None, split), P(None, split), P(None, split), P(None, split),
        P(None, split), P(None, split), P(split), P(split), P(split, None), P(split), P(split, None),
    )
    return jax.shard_map(
        functools.partial(local, mesh.shape["mesh"]), mesh=mesh, in_specs=in_specs, out_specs=P(None, None, split), check_vma=False
    )
```

```python
import functools
import math

import jax
import jax.numpy as jnp
from jax import lax
from jax.experimental import pallas as pl
from jax.experimental.pallas import tpu as pltpu
from jax.sharding import PartitionSpec as P

STEPS = 2
DT = 0.1
TOPMOST = lax.Precision.HIGHEST
LANES = 128
CHUNK = 256
F32, BF16 = jnp.float32, jnp.bfloat16


def halves(x):
    high = x.astype(BF16)
    return high, (x - high.astype(F32)).astype(BF16)


def dot(a, b):
    return jnp.dot(a, b, preferred_element_type=F32)


def merge_slots(ids, weights):
    ids, weights = list(ids), [list(w) for w in weights]
    for s in range(1, len(ids)):
        for t in range(s):
            same = ids[s] == ids[t]
            for w in weights:
                w[t] = w[t] + jnp.where(same, w[s], 0.0)
            ids[s] = jnp.where(same, -1, ids[s])
    return ids, weights


def build(out_ref, places, extent, ids_ref, parts_ref, slots, kinds):
    columns = ids_ref.shape[1]
    rows = 16

    def column(c, _):
        cols = pl.ds(pl.multiple_of(c * LANES, LANES), LANES)
        ids = [jnp.broadcast_to(ids_ref[s : s + 1, cols], (rows, LANES)).astype(jnp.int16) for s in range(slots)]
        parts = [
            [jnp.broadcast_to(parts_ref[q * slots + s : q * slots + s + 1, cols], (rows, LANES)).astype(BF16) for s in range(slots)]
            for q in range(kinds)
        ]
        blank = jnp.zeros((rows, LANES), BF16)

        unroll = 4

        def block(r, _):
            for u in range(unroll):
                start = pl.multiple_of((r * unroll + u) * rows, rows)
                here = places + jnp.full((rows, LANES), start, jnp.int32).astype(jnp.int16)
                total = [blank] * kinds
                for s in range(slots):
                    hit = here == ids[s]
                    total = [jnp.where(hit, parts[q][s], total[q]) for q in range(kinds)]
                for q in range(kinds):
                    out_ref[q, pl.ds(start, rows), cols] = total[q]
            return 0

        lax.fori_loop(0, extent // (rows * unroll), block, 0)
        return 0

    lax.fori_loop(0, columns // LANES, column, 0)


def linv_of(table, unit, members):
    width = 8
    work = jnp.concatenate([table, unit], axis=1)
    count = members // width
    blocks = [work[b * width : (b + 1) * width] for b in range(count)]
    done = []
    for b in range(count):
        first = b * width
        panel = blocks[b]
        full = (width, work.shape[1])
        rows = [jnp.broadcast_to(panel[j : j + 1], full) for j in range(width)]
        corner = {
            (j, i): jnp.broadcast_to(panel[j : j + 1, first + i : first + i + 1], full)
            for j in range(width) for i in range(j, width)
        }
        scaled, scales = [], {}
        for j in range(width):
            inverse = 1.0 / corner[j, j]
            scaled.append(rows[j] * inverse)
            for i in range(j + 1, width):
                scales[j, i] = corner[j, i] * inverse
            for i in range(j + 1, width):
                rows[i] = rows[i] - scales[j, i] * rows[j]
                for k in range(i, width):
                    corner[i, k] = corner[i, k] - scales[j, i] * corner[j, k]
        for j in range(width):
            done.append((rows[j] * lax.rsqrt(corner[j, j]))[:1])
        if b + 1 < count:
            for j in reversed(range(width)):
                for i in range(j + 1, width):
                    scaled[j] = scaled[j] - scales[j, i] * scaled[i]
        for n in range(b + 1, count):
            total = blocks[n]
            for j in range(width):
                total = total - blocks[n][:, first + j : first + j + 1] * scaled[j]
            blocks[n] = total
    return jnp.concatenate(done, axis=0)[:, members:]


def kernel(
    n, state, depth, coef, wet, conn, lists, obs_nodes, obs_weight, obs_value, obs_error, loc_ids, loc_len, loc_weight,
    out, field, operator, picker, sampler, slot_ids, slot_parts, obs_ids, obs_parts, totals, mixed, gather_mixed,
    sums, send_flow, got_flow, send_level, got_level, shares, got_shares, grams, got_grams, anomalies, send_sem, recv_sem,
):
    me = lax.axis_index("mesh")
    lower, upper = lax.rem(me + n - 1, n), lax.rem(me + 1, n)
    has_lower, has_upper = me > 0, me < n - 1
    members, nodes = state.shape[1], state.shape[2]
    slots, corners = conn.shape[0], obs_nodes.shape[0]
    width = lists.shape[1]
    extent = nodes + 2 * width
    obs_count = obs_value.shape[1]

    barrier = pltpu.get_barrier_semaphore()

    @pl.when(has_lower)
    def _():
        pl.semaphore_signal(barrier, inc=1, device_id={"mesh": lower}, device_id_type=pl.DeviceIdType.MESH)

    @pl.when(has_upper)
    def _():
        pl.semaphore_signal(barrier, inc=1, device_id={"mesh": upper}, device_id_type=pl.DeviceIdType.MESH)

    def pair(k, source, target):
        down = pltpu.make_async_remote_copy(
            src_ref=source.at[0], dst_ref=target.at[1], send_sem=send_sem.at[k, 0], recv_sem=recv_sem.at[k, 0],
            device_id={"mesh": lower}, device_id_type=pl.DeviceIdType.MESH,
        )
        up = pltpu.make_async_remote_copy(
            src_ref=source.at[1], dst_ref=target.at[0], send_sem=send_sem.at[k, 1], recv_sem=recv_sem.at[k, 1],
            device_id={"mesh": upper}, device_id_type=pl.DeviceIdType.MESH,
        )
        return down, up

    def start(copies):
        pl.when(has_lower)(copies[0].start)
        pl.when(has_upper)(copies[1].start)

    def arrive(copies):
        pl.when(has_upper)(copies[0].wait_recv)
        pl.when(has_lower)(copies[1].wait_recv)

    def sent(copies):
        pl.when(has_lower)(copies[0].wait_send)
        pl.when(has_upper)(copies[1].wait_send)

    flow_copies = [pair(i, send_flow.at[i], got_flow.at[i]) for i in range(STEPS)]
    level_copies = [pair(STEPS + i, send_level.at[i], got_level.at[i]) for i in range(STEPS)]
    share_copies = pair(2 * STEPS, shares, got_shares)
    gram_copies = pair(2 * STEPS + 1, grams, got_grams)

    def blank_side(side):
        for i in range(STEPS):
            got_flow[i, side] = jnp.zeros_like(got_flow[i, side])
            got_level[i, side] = jnp.zeros_like(got_level[i, side])
        got_shares[side] = jnp.zeros_like(got_shares[side])
        got_grams[side] = jnp.zeros_like(got_grams[side])

    pl.when(me == 0)(lambda: blank_side(0))
    pl.when(me == n - 1)(lambda: blank_side(1))

    places = lax.broadcasted_iota(jnp.int32, (16, LANES), 0).astype(jnp.int16)

    def pick_column(c, _):
        cols = pl.ds(pl.multiple_of(c * LANES, LANES), LANES)
        for h in range(2):
            ids = jnp.broadcast_to(lists[h : h + 1, cols], (16, LANES)).astype(jnp.int16)

            def block(r, _):
                begin = pl.multiple_of(r * 16, 16)
                here = places + jnp.full((16, LANES), begin, jnp.int32).astype(jnp.int16)
                picker[h, pl.ds(begin, 16), cols] = jnp.where(here == ids, jnp.ones((16, LANES), BF16), jnp.zeros((16, LANES), BF16))
                return 0

            lax.fori_loop(0, nodes // 16, block, 0, unroll=4)
        return 0

    lax.fori_loop(0, width // LANES, pick_column, 0)

    def split_field(f, values, cols):
        high, low = halves(values)
        mixed[2 * f * members : (2 * f + 1) * members, cols] = high
        mixed[(2 * f + 1) * members : (2 * f + 2) * members, cols] = low

    def send_fields(first, number, target):
        for h in range(2):
            picked = dot(mixed[2 * first * members : 2 * (first + number) * members, :], picker[h])
            for f in range(number):
                base = 2 * f * members
                target[h, f * members : (f + 1) * members, :] = (
                    picked[base : base + members] + picked[base + members : base + 2 * members]
                )

    def over_chunks(body):
        def step(c, _):
            body(pl.ds(pl.multiple_of(c * CHUNK, CHUNK), CHUNK))
            return 0

        lax.fori_loop(0, nodes // CHUNK, step, 0)

    def product(pairs_ref, base, op, rows, cols):
        both = dot(pairs_ref[base : base + 2 * members, :], operator[2 * op, rows, cols])
        cross = dot(pairs_ref[base : base + members, :], operator[2 * op + 1, rows, cols])
        return both[:members] + both[members:] + cross

    local_rows, ghost_rows = slice(0, nodes), slice(nodes, extent)

    def first_split(cols):
        for f in (1, 2):
            split_field(f, state[f, :, cols], cols)

    over_chunks(first_split)
    send_fields(1, 2, send_flow.at[0])

    pl.semaphore_wait(barrier, jnp.minimum(me, 1) + jnp.minimum(n - 1 - me, 1))
    start(flow_copies[0])

    list_size = loc_ids.shape[1]
    groups = 3 * obs_count // LANES
    live = lax.broadcasted_iota(jnp.int32, (1, list_size), 1) < loc_len[0]
    entry = jnp.where(live, loc_weight[...], 0.0)
    position = loc_ids[...] - (me - 1) * obs_count
    major, minor = position // LANES, lax.rem(position, LANES)
    coarse = jnp.where(lax.broadcasted_iota(jnp.int32, (groups, list_size), 0) == major, entry, 0.0)
    fine = jnp.where(lax.broadcasted_iota(jnp.int32, (LANES, list_size), 0) == minor, 1.0, 0.0)
    dense = lax.dot_general(coarse, fine, (((1,), (1,)), ((), ())), precision=TOPMOST, preferred_element_type=F32)
    third = groups // 3
    shares[0] = dense[:third]
    shares[1] = dense[2 * third :]
    own_share = dense[third : 2 * third]
    start(share_copies)

    faces = wet[...].astype(F32)
    east, north = faces * coef[:, 0], faces * coef[:, 1]
    totals[0:1] = jnp.sum(east, axis=0, keepdims=True)
    totals[1:2] = jnp.sum(north, axis=0, keepdims=True)
    ids, (east_slots, north_slots) = merge_slots(
        [conn[s : s + 1] for s in range(slots)],
        [[east[s : s + 1] for s in range(slots)], [north[s : s + 1] for s in range(slots)]],
    )
    for s in range(slots):
        slot_ids[s : s + 1] = ids[s]
        for q, w in enumerate((east_slots[s], north_slots[s])):
            high, low = halves(w)
            slot_parts[2 * q * slots + s : 2 * q * slots + s + 1] = high.astype(F32)
            slot_parts[(2 * q + 1) * slots + s : (2 * q + 1) * slots + s + 1] = low.astype(F32)
    build(operator, places, extent, slot_ids, slot_parts, slots, 4)

    ids, (weight_slots,) = merge_slots(
        [obs_nodes[s : s + 1] for s in range(corners)], [[obs_weight[s : s + 1] for s in range(corners)]]
    )
    for s in range(corners):
        obs_ids[s : s + 1] = ids[s]
        high, low = halves(weight_slots[s])
        obs_parts[s : s + 1] = high.astype(F32)
        obs_parts[corners + s : corners + s + 1] = low.astype(F32)

    for i in range(STEPS):
        old = state if i == 0 else field
        last = i == STEPS - 1

        def flow_local(cols, old=old):
            sums[0, :, cols] = (
                product(mixed, 2 * members, 0, local_rows, cols)
                + product(mixed, 4 * members, 1, local_rows, cols)
                - old[1, :, cols] * totals[0:1, cols]
                - old[2, :, cols] * totals[1:2, cols]
            )

        over_chunks(flow_local)
        if i == 0:
            build(sampler, places, nodes, obs_ids, obs_parts, corners, 2)
        arrive(flow_copies[i])
        for side in range(2):
            for f in range(2):
                high, low = halves(got_flow[i, side, f * members : (f + 1) * members, :])
                gather_mixed[2 * f * members : (2 * f + 1) * members, side * width : (side + 1) * width] = high
                gather_mixed[(2 * f + 1) * members : (2 * f + 2) * members, side * width : (side + 1) * width] = low

        def flow_ghost(cols, old=old):
            divergence = (
                sums[0, :, cols]
                + product(gather_mixed, 0, 0, ghost_rows, cols)
                + product(gather_mixed, 2 * members, 1, ghost_rows, cols)
            )
            level = old[0, :, cols] - DT * depth[0:1, cols] * divergence
            field[0, :, cols] = level
            split_field(0, level, cols)

        over_chunks(flow_ghost)
        send_fields(0, 1, send_level.at[i])
        start(level_copies[i])

        if last:
            arrive(share_copies)

            def observe(cols):
                both = dot(mixed[: 2 * members, :], sampler[0, :, cols])
                observed = both[:members] + both[members:] + dot(mixed[:members, :], sampler[1, :, cols])
                mean = jnp.mean(observed, axis=0, keepdims=True)
                anomalies[:members, cols] = observed - mean
                anomalies[members : members + 8, cols] = jnp.broadcast_to(obs_value[0:1, cols] - mean, (8, CHUNK))

            over_chunks(observe)
            precision = 1.0 / (obs_error[...] * obs_error[...])
            scaled = []
            for share in (got_shares[0], own_share, got_shares[1]):
                line = jnp.concatenate([share[a : a + 1] for a in range(third)], axis=1)
                scaled.append(anomalies[...] * (line * precision))
            table = lax.dot_general(
                jnp.concatenate(scaled, axis=0), anomalies[:members], (((1,), (1,)), ((), ())),
                precision=TOPMOST, preferred_element_type=F32,
            )
            tall = members + 8
            pad = jnp.zeros((tall, grams.shape[2] - members), F32)
            grams[0] = jnp.concatenate([table[:tall], pad], axis=1)
            grams[1] = jnp.concatenate([table[2 * tall :], pad], axis=1)
            own_table = table[tall : 2 * tall]
            start(gram_copies)

        def level_local(cols):
            level = field[0, :, cols]
            for d in range(2):
                sums[d, :, cols] = product(mixed, 0, d, local_rows, cols) - level * totals[d : d + 1, cols]

        over_chunks(level_local)
        arrive(level_copies[i])
        for side in range(2):
            high, low = halves(got_level[i, side])
            gather_mixed[:members, side * width : (side + 1) * width] = high
            gather_mixed[members : 2 * members, side * width : (side + 1) * width] = low

        def level_ghost(cols, old=old, last=last):
            for d in range(2):
                slope = sums[d, :, cols] + product(gather_mixed, 0, d, ghost_rows, cols)
                value = old[1 + d, :, cols] - DT * slope
                field[1 + d, :, cols] = value
                if not last:
                    split_field(1 + d, value, cols)

        over_chunks(level_ghost)
        if not last:
            send_fields(1, 2, send_flow.at[i + 1])
            start(flow_copies[i + 1])

    arrive(gram_copies)
    combined = own_table + got_grams[0, :, :members] + got_grams[1, :, :members]
    unit = jnp.where(
        lax.broadcasted_iota(jnp.int32, (members, members), 0) == lax.broadcasted_iota(jnp.int32, (members, members), 1), 1.0, 0.0
    )
    linv = linv_of(combined[:members] + (members - 1.0) * unit, unit, members)
    rhs = combined[members : members + 1]
    halfway = jnp.sum(linv * rhs, axis=1, keepdims=True)
    mean_w = jnp.sum(linv * halfway, axis=0, keepdims=True)
    blend = mean_w + math.sqrt(members - 1.0) * linv

    def analyse(cols):
        for c in range(3):
            forecast = field[c, :, cols]
            average = jnp.mean(forecast, axis=0, keepdims=True)
            out[c, :, cols] = average + jnp.dot(blend, forecast - average, precision=TOPMOST, preferred_element_type=F32)

    over_chunks(analyse)
    for copies in flow_copies + level_copies + [share_copies, gram_copies]:
        sent(copies)


def local(
    n, state, depth, coef, wet_faces, conn, send_list, obs_nodes, obs_weight, obs_value, obs_error, loc_ids, loc_len, loc_weight
):
    members, nodes = state.shape[1], state.shape[2]
    slots, corners, width = conn.shape[0], obs_nodes.shape[0], send_list.shape[1]
    obs_count = obs_value.shape[0]
    extent = nodes + 2 * width
    assert loc_ids.shape[0] == 1
    vmem = pl.BlockSpec(memory_space=pltpu.VMEM)
    smem = pl.BlockSpec(memory_space=pltpu.SMEM)
    number = 2 * STEPS + 2
    return pl.pallas_call(
        functools.partial(kernel, n),
        out_shape=jax.ShapeDtypeStruct(state.shape, F32),
        in_specs=[vmem] * 11 + [smem, vmem],
        out_specs=vmem,
        scratch_shapes=[
            pltpu.VMEM((3, members, nodes), F32),
            pltpu.VMEM((4, extent, nodes), BF16),
            pltpu.VMEM((2, nodes, width), BF16),
            pltpu.VMEM((2, nodes, obs_count), BF16),
            pltpu.VMEM((8, nodes), jnp.int32),
            pltpu.VMEM((4 * slots, nodes), F32),
            pltpu.VMEM((8, obs_count), jnp.int32),
            pltpu.VMEM((8, obs_count), F32),
            pltpu.VMEM((8, nodes), F32),
            pltpu.VMEM((6 * members, nodes), BF16),
            pltpu.VMEM((4 * members, 2 * width), BF16),
            pltpu.VMEM((2, members, nodes), F32),
            pltpu.VMEM((STEPS, 2, 2 * members, width), F32),
            pltpu.VMEM((STEPS, 2, 2 * members, width), F32),
            pltpu.VMEM((STEPS, 2, members, width), F32),
            pltpu.VMEM((STEPS, 2, members, width), F32),
            pltpu.VMEM((2, obs_count // LANES, LANES), F32),
            pltpu.VMEM((2, obs_count // LANES, LANES), F32),
            pltpu.VMEM((2, members + 8, LANES), F32),
            pltpu.VMEM((2, members + 8, LANES), F32),
            pltpu.VMEM((members + 8, obs_count), F32),
            pltpu.SemaphoreType.DMA((number, 2)),
            pltpu.SemaphoreType.DMA((number, 2)),
        ],
        compiler_params=pltpu.CompilerParams(collective_id=0, has_side_effects=True, vmem_limit_bytes=56 * 1024 * 1024),
    )(
        state, depth[None], jnp.swapaxes(coef, 0, 1), wet_faces, conn, send_list, obs_nodes, obs_weight, obs_value[None], obs_error[None],
        loc_ids, loc_len, loc_weight,
    )


def solution(mesh):
    split = ("groups", "mesh")
    in_specs = (
        P(None, None, split), P(split), P(None, None, split), P(None, split), P(None, split), P(None, split),
        P(None, split), P(None, split), P(split), P(split), P(split, None), P(split), P(split, None),
    )
    return jax.shard_map(
        functools.partial(local, mesh.shape["mesh"]), mesh=mesh, in_specs=in_specs, out_specs=P(None, None, split), check_vma=False
    )
```
